32 devices in a mesh: grow: 8 (over y, x, core), gcol: 4 (over z).
Axes of the slice: x: 2, y: 2, z: 4, core: 2. Of those that a mesh axis runs over, the one named last changes fastest.
Arguments:
- eps_static: float32 [12288, 12288], P('grow', 'gcol'), may hold values from -1.8 to 1.8
- eps_imag: float32 [12288, 12288], P('grow', 'gcol'), may hold values from -1.8 to 1.8
- frequency_grid: float32 [3], replicated, may hold values from 0.1 to 2
- band_energy: float32 [32], replicated, may hold values from -2 to 2
- pair_elements: bfloat16 [32, 64, 12288], P('grow', None, 'gcol'), may hold values from -0.0546875 to 0.0546875
Outputs:
- sigma: float32 [3, 64], P(None, 'gcol')
The draws below stay inside these ranges and needn't reach their ends.
All inputs are finite; a program needn't handle non-finite values.
Results may differ from the reference program's by a relative error of at most 0.0019.
Values may be sent and summed in bfloat16 or wider, within the bound.
A program may use at most 128 MiB of HBM per device.

```python
import math
import jax
import jax.numpy as jnp
from jax import lax

NG = 12288
STATES = 64
BANDS = 32
NE = 3


def block_levels(key, extent, cuts, low, high):
    level, own = 1.0, jax.random.fold_in(key, 6)
    for position, parts in cuts:
        heights = jnp.exp(jax.random.uniform(jax.random.fold_in(own, position), (parts,), jnp.float32, low / len(cuts), high / len(cuts)))
        level = level * jnp.repeat(heights, extent[position] // parts).reshape([-1 if axis == position else 1 for axis in range(len(extent))])
    return level


def gaussian(own_key, dims, scale, limit, cuts=(), kind=jnp.bfloat16):
    entries = scale * jax.random.normal(own_key, dims, jnp.float32)
    if cuts:
        entries = entries * block_levels(own_key, dims, cuts, -0.22, 0.18)
    return jnp.clip(entries, -limit, limit).astype(kind)


def setup_inputs(seed: int = 0) -> dict:
    arg_keys = jax.random.split(jax.random.key(seed), 6)
    eps_static = gaussian(arg_keys[0], (NG, NG), 0.3, 1.8, ((0, 8), (1, 4)), jnp.float32)
    eps_imag = gaussian(arg_keys[1], (NG, NG), 0.3, 1.8, ((0, 8), (1, 4)), jnp.float32)
    frequency_grid = jnp.clip(jnp.exp(jax.random.uniform(arg_keys[2], (NE,), jnp.float32, math.log(0.1), math.log(2.0))), 0.1, 2.0)
    band_energy = jnp.clip(jax.random.uniform(arg_keys[3], (BANDS,), jnp.float32, -2.0, 2.0), -2.0, 2.0)
    pair_elements = gaussian(arg_keys[4], (BANDS, STATES, NG), NG ** -0.5, 0.0546875, ((0, 8), (2, 4)))
    return dict(eps_static=eps_static, eps_imag=eps_imag, frequency_grid=frequency_grid, band_energy=band_energy, pair_elements=pair_elements)


def pole_kernels(static_rows, imag_rows, kronecker, frequency_grid):
    static_part = static_rows - kronecker
    imag_part = imag_rows - kronecker
    spread = static_part - imag_part
    pole_square = (imag_part * imag_part + 0.25) / (spread * spread + 0.25)
    pole_freq = jnp.sqrt(pole_square)
    strength = -static_part * pole_square
    return [(strength / (pole_freq * (pole_freq + frequency_grid[point]))).astype(jnp.bfloat16) for point in range(NE)]

def reference(eps_static, eps_imag, frequency_grid, band_energy, pair_elements):
    blocks = 16
    height = NG // blocks
    rows_all = pair_elements.reshape(BANDS * STATES, NG).astype(jnp.float32)
    col_ids = lax.iota(jnp.int32, NG)
    row_ids = lax.iota(jnp.int32, height)

    def advance(block, quad):
        start = (block * height).astype(jnp.int32)
        static_rows = lax.dynamic_slice_in_dim(eps_static, start, height, 0)
        imag_rows = lax.dynamic_slice_in_dim(eps_imag, start, height, 0)
        kronecker = ((start + row_ids)[:, None] == col_ids[None, :]).astype(jnp.float32)
        kernels = pole_kernels(static_rows, imag_rows, kronecker, frequency_grid)
        left = lax.dynamic_slice_in_dim(rows_all, start, height, 1)
        terms = []
        for kernel in kernels:
            wide = lax.optimization_barrier(kernel).astype(jnp.float32)
            projected = jnp.dot(left, wide, precision=lax.Precision.HIGHEST)
            terms.append(lax.optimization_barrier(jnp.sum(projected * rows_all, axis=1)))
        return quad + jnp.stack(terms)
    quad = lax.fori_loop(0, blocks, advance, jnp.zeros((NE, BANDS * STATES), jnp.float32))
    quad = quad.reshape(NE, BANDS, STATES)
    offset = frequency_grid[:, None] - band_energy[None, :]
    weight = 1.0 / (1.0 + offset * offset)
    return jnp.einsum('em,ems->es', weight, quad)
```

```python
import functools

import jax
import jax.numpy as jnp
from jax import lax
from jax.experimental import pallas as pl
from jax.experimental.pallas import tpu as pltpu
from jax.sharding import PartitionSpec as P

LANES = 128
SUB_ROWS = 32
SUB_COLS = 512
DOT_ROWS = 128
DOT_COLS = 1536
BUILD_RATE = 2
PIECE_RATE = 2
LEAD = 4


def bit_flip(index, mask, extent):
    total, bit = 0, 1
    while bit < extent:
        total = total + ((index // bit + mask // bit) % 2) * bit
        bit *= 2
    return total


def flag(condition):
    return jnp.where(condition, 1, 0)


def count(table, tick):
    total = 0
    for entry in table:
        total = total + flag(tick >= entry)
    return total


def look(table, index):
    value = table[0]
    for n in range(1, len(table)):
        value = jnp.where(index >= n, table[n], value)
    return value


def rising(ticks):
    out = []
    for tick in ticks:
        out.append(max(tick, out[-1] if out else tick))
    return out


class Plan:
    def __init__(self, R, Z, bpd, states, breadth, blocks):
        ratio = R // Z
        self.mains, self.asides = (R - ratio) * bpd, ratio * bpd
        levels = {}
        for shard in range(R):
            levels.setdefault(bin(shard // 2).count("1"), []).append(shard)
        self.col_order, self.col_ticks = [], []
        tick = 0
        for level in sorted(levels):
            shards = sorted(levels[level], key=lambda shard: (shard % 2, shard))
            if level == 0:
                found = [b + bpd * shard for shard in shards for b in range(bpd)]
                ticks = [n // 4 for n in range(len(found))]
                tick = 2 * bpd // 2
            else:
                found = [b + bpd * shard for b in range(bpd) for shard in shards]
                each = 2 if level == 1 else 1
                ticks = [tick + n // each for n in range(len(found))]
                tick = ticks[-1] + 1
            self.col_order += found
            self.col_ticks += ticks
        due = dict(zip(self.col_order, self.col_ticks))
        main_due = [due[j] if j < ratio * bpd else max(due[j], due[j + ratio * bpd]) for j in range(self.mains)]
        self.home_ticks = rising([max(0, j - LEAD, main_due[j]) for j in range(self.mains)])
        aside_due = [max(due[k + bpd * ratio * c] for c in range(1, Z)) for k in range(self.asides)]
        step = Z - 1
        early = 2
        self.relay_pass, self.relay_end = [], []
        for d in range(Z):
            self.relay_pass.append([2 * d + (i if i <= early else early + step * (i - early) - 1) for i in range(self.asides)])
            spread = [step * i + d + 1 for i in range(self.asides)]
            self.relay_end.append(rising([max(tick, 4 * d - 3 + 2 * i) if d else tick for i, tick in enumerate(spread)]))
        self.aside_ticks = rising([max(t[k] for t in self.relay_end[1:]) + 3 for k in range(self.asides)])
        self.gb = max(1, min(bpd, DOT_ROWS // states))
        self.gps = bpd // self.gb
        found = []
        for g in range(self.mains // self.gb):
            units = range(g * self.gb, (g + 1) * self.gb)
            found.append((units[-1], max(main_due[j] for j in units), 2 * g))
        for g in range(self.asides // self.gb):
            units = range(g * self.gb, (g + 1) * self.gb)
            found.append((0, max([self.aside_ticks[units[-1]]] + [aside_due[k] for k in units]), 2 * g + 1))
        found.sort(key=lambda entry: (max(entry[0] + 2, entry[1]), entry[0]))
        self.groups = [entry[2] for entry in found]
        self.row_need = rising([entry[0] for entry in found])
        self.col_need = rising([entry[1] for entry in found])
        self.ticks = max(self.mains + Z + 1, self.row_need[-1] + Z + 2, self.col_need[-1] + 2,
                         max(t[-1] for t in self.relay_pass) + 1, max(t[-1] for t in self.relay_end) + 1)
        self.build_ticks = -(-blocks // BUILD_RATE)


def body(R, Z, bpd, states, height, breadth, ne,
         freq, energy, es_hbm, ei_hbm, pair_hbm, out,
         kern, colp, rowp, es_buf, ei_buf, sig, part, recv1, recv2, hold,
         eps_sem, own_sem, col_send, col_recv, row_recv, up_send, dn_send,
         s1_send, s1_recv, s2_send, s2_recv, hold_send, hold_recv, give_send):
    r = lax.axis_index("grow")
    z = lax.axis_index("gcol")
    ratio = R // Z
    home = r // ratio
    core = r % ratio
    offset = pl.multiple_of(core * height, height)
    spc = states // Z
    units = R * bpd
    blocks = 4 * bpd
    rows = height // blocks
    plan = Plan(R, Z, bpd, states, breadth, blocks)

    def dev(row, col):
        return dict(device_id={"grow": row, "gcol": col}, device_id_type=pl.DeviceIdType.MESH)

    def eps_copies(block, slot):
        at = pl.multiple_of(block * rows, rows)
        return (pltpu.make_async_copy(es_hbm.at[pl.ds(at, rows), :], es_buf.at[slot], eps_sem.at[0, slot]),
                pltpu.make_async_copy(ei_hbm.at[pl.ds(at, rows), :], ei_buf.at[slot], eps_sem.at[1, slot]))

    own = pltpu.make_async_copy(pair_hbm, colp.at[0], own_sem)
    own.start()
    for copy in eps_copies(0, 0):
        copy.start()

    barrier = pltpu.get_barrier_semaphore()
    for d in range(1, R):
        pl.semaphore_signal(barrier, inc=1, **dev((r + d) % R, z))
    for d in range(1, Z):
        pl.semaphore_signal(barrier, inc=1, **dev(r, (z + d) % Z))
    sig[...] = jnp.zeros_like(sig)
    own.wait()
    pl.semaphore_wait(barrier, R + Z - 2)

    def unit_rows(b):
        return pl.ds(pl.multiple_of(b * states, states), states)

    def col_copy(src_shard, dst_shard, b, row, sems=0):
        return pltpu.make_async_remote_copy(
            src_ref=colp.at[src_shard, unit_rows(b), :], dst_ref=colp.at[dst_shard, unit_rows(b), :],
            send_sem=col_send.at[sems * units + dst_shard * bpd + b], recv_sem=col_recv.at[dst_shard * bpd + b],
            **dev(row, z))

    partner = bit_flip(r, 1, R)
    bits = []
    while 2 ** (len(bits) + 1) < R:
        bits.append(2 ** (len(bits) + 1))

    top = bits[-1] if bits else 1
    heavy = jnp.where(2 * z < Z, 0, Z - 1)
    is_heavy = home == heavy

    def backward(shard):
        return (r // top + shard // top) % 2 == (heavy * ratio // top) % 2

    def send_own(b, carry):
        for bit in [1] + bits[1:]:
            col_copy(0, bit, b, bit_flip(r, bit, R)).start()
        return carry
    lax.fori_loop(0, bpd, send_own, 0)

    def send_near(b, carry):
        col_copy(0, bits[0], b, bit_flip(r, bits[0], R)).start()
        return carry

    at_home = z == home
    goes_up = jnp.logical_and(z >= home, z < Z - 1)
    goes_down = jnp.logical_and(z <= home, z > 0)
    upper = (z + 1) % Z
    lower = (z + Z - 1) % Z
    hops = jnp.where(z > home, z - home, home - z)
    lag = jnp.where(at_home, 0, hops + 1)
    skip_up = bit_flip(home, Z - 1, Z) * ratio
    skip_down = home * ratio
    skip = jnp.where(at_home, R - ratio, jnp.where(z < home, skip_down, skip_up))

    def main_shard(m, skipped):
        return m + ratio * flag(m >= skipped)

    def aside_shard(a):
        return skip + a

    def row_copy(shard, b, sems, col):
        u = shard * bpd + b
        ref = rowp.at[shard, unit_rows(b), :]
        return pltpu.make_async_remote_copy(
            src_ref=ref, dst_ref=ref, send_sem=sems.at[u], recv_sem=row_recv.at[u], **dev(r, col))

    def home_copy(shard, b, sems, col):
        u = shard * bpd + b
        return pltpu.make_async_remote_copy(
            src_ref=colp.at[shard, unit_rows(b), pl.ds(offset, height)], dst_ref=rowp.at[shard, unit_rows(b), :],
            send_sem=sems.at[u], recv_sem=row_recv.at[u], **dev(r, col))

    def col_event(n, carry):
        u = look(plan.col_order, n)
        shard, b = u // bpd, u % bpd

        @pl.when(shard >= 1)
        def _():
            col_copy(0, shard, b, partner).wait_recv()

        @pl.when(jnp.logical_and(shard >= 2, shard % 2 == 0))
        def _():
            col_copy(shard, shard + 1, b, partner).start()
            for bit in bits[1:]:
                @pl.when(jnp.logical_and(shard < bit, jnp.logical_not(backward(shard))))
                def _(bit=bit):
                    col_copy(shard, shard + bit, b, bit_flip(r, bit, R)).start()
            for bit in bits[:-1]:
                @pl.when(jnp.logical_and(shard % (2 * bit) == 0, backward(shard)))
                def _(bit=bit):
                    col_copy(shard, shard + bit, b, bit_flip(r, bit, R), 1).start()

        @pl.when(at_home)
        def _():
            local = pltpu.make_async_copy(
                colp.at[shard, unit_rows(b), pl.ds(offset, height)],
                rowp.at[shard, unit_rows(b), :], row_recv.at[u])
            local.start()
            local.wait()
        return carry

    def home_event(j, carry):
        m, b = j // bpd, j % bpd

        @pl.when(goes_up)
        def _():
            home_copy(main_shard(m, skip_up), b, up_send, upper).start()

        @pl.when(goes_down)
        def _():
            home_copy(main_shard(m, skip_down), b, dn_send, lower).start()
        return carry

    def main_event(j, carry):
        shard, b = main_shard(j // bpd, skip), j % bpd
        row_copy(shard, b, up_send, upper).wait_recv()

        @pl.when(goes_up)
        def _():
            row_copy(shard, b, up_send, upper).start()

        @pl.when(goes_down)
        def _():
            row_copy(shard, b, dn_send, lower).start()
        return carry

    def aside_event(k, carry):
        row_copy(aside_shard(k // bpd), k % bpd, up_send, upper).wait_recv()
        return carry

    relay_down = home == 0
    relays = jnp.logical_or(relay_down, home == Z - 1)
    ahead = jnp.where(relay_down, z - 1, z + 1)
    has_ahead = jnp.logical_and(relays, jnp.logical_and(ahead >= 0, ahead < Z))
    ahead_col = (ahead + Z) % Z
    ends = jnp.logical_and(relays, jnp.logical_not(has_ahead))

    def hold_rows(i):
        return pl.ds(pl.multiple_of(i * states, states), states)

    def hold_copy(d, i):
        if d == 0:
            src = colp.at[i // bpd, unit_rows(i % bpd), pl.ds(offset, height)]
        else:
            src = hold.at[d - 1, hold_rows(i), :]
        return pltpu.make_async_remote_copy(
            src_ref=src, dst_ref=hold.at[min(d, Z - 2), hold_rows(i), :],
            send_sem=hold_send.at[d * plan.asides + i], recv_sem=hold_recv.at[min(d, Z - 2) * plan.asides + i],
            **dev(r, ahead_col))

    def give_copy(d, i, panel):
        to = panel * ratio + core
        shard = bit_flip(panel, home, Z) * ratio + i // bpd
        return pltpu.make_async_remote_copy(
            src_ref=hold.at[d - 1, hold_rows(i), :], dst_ref=rowp.at[shard, unit_rows(i % bpd), :],
            send_sem=give_send.at[(d - 1) * plan.asides + i], recv_sem=row_recv.at[shard * bpd + i % bpd],
            **dev(to, z))

    def panel_of(d):
        return jnp.where(relay_down, z + d, z - d)

    def holds(d):
        return jnp.logical_and(relays, jnp.logical_and(panel_of(d) >= 0, panel_of(d) < Z))

    def relay(tick):
        for d in range(Z):
            def item(i, carry, d=d):
                if d == 0:
                    hold_copy(d, i).start()
                    return carry
                hold_copy(d - 1, i).wait_recv()

                @pl.when(has_ahead)
                def _():
                    hold_copy(d, i).start()
                give_copy(d, i, (panel_of(d) + Z) % Z).start()
                return carry

            passing = (count(plan.relay_pass[d], tick - 1), count(plan.relay_pass[d], tick))
            if d == 0:
                live = has_ahead
                lo, hi = passing
            else:
                live = holds(d)
                lo = jnp.where(ends, count(plan.relay_end[d], tick - 1), passing[0])
                hi = jnp.where(ends, count(plan.relay_end[d], tick), passing[1])

            @pl.when(jnp.logical_and(live, hi > lo))
            def _():
                lax.fori_loop(lo, hi, item, 0)

    diagonal = r * height - z * breadth
    sub_rows = min(SUB_ROWS, rows)
    sub_cols = min(SUB_COLS, breadth)
    col_steps = breadth // sub_cols
    f0, f1, f2 = freq[0], freq[1], freq[2]

    def make_block(block, carry):
        slot = block % 2

        @pl.when(block + 1 < blocks)
        def _():
            for copy in eps_copies(block + 1, 1 - slot):
                copy.start()
        for copy in eps_copies(block, slot):
            copy.wait()
        base = pl.multiple_of(block * rows, rows)

        def chunk(n, carry):
            at_row = pl.multiple_of(n // col_steps * sub_rows, sub_rows)
            at_col = pl.multiple_of(n % col_steps * sub_cols, sub_cols)
            where = (pl.ds(at_row, sub_rows), pl.ds(at_col, sub_cols))
            gap = (lax.broadcasted_iota(jnp.int32, (sub_rows, sub_cols), 0)
                   - lax.broadcasted_iota(jnp.int32, (sub_rows, sub_cols), 1))
            one = jnp.where(gap == at_col - at_row - base - diagonal, 1.0, 0.0)
            static = es_buf[(slot,) + where] - one
            imag = ei_buf[(slot,) + where] - one
            spread = static - imag
            over = imag * imag + 0.25
            under = spread * spread + 0.25
            pole = over * lax.rsqrt(over * under)
            p0, p1, p2 = pole + f0, pole + f1, pole + f2
            p01 = p0 * p1
            scale = -static * pole / (p01 * p2)
            to = (pl.ds(pl.multiple_of(base + at_row, sub_rows), sub_rows), where[1])
            kern[(0,) + to] = (p1 * p2 * scale).astype(jnp.bfloat16)
            kern[(1,) + to] = (p0 * p2 * scale).astype(jnp.bfloat16)
            kern[(2,) + to] = (p01 * scale).astype(jnp.bfloat16)
            return carry
        lax.fori_loop(0, rows // sub_rows * col_steps, chunk, 0)
        return carry

    gb, gps = plan.gb, plan.gps
    group_rows = gb * states
    dot_cols = min(DOT_COLS, breadth)
    while breadth % dot_cols:
        dot_cols //= 2
    cuts = breadth // dot_cols

    def piece(number, carry):
        code, q = look(plan.groups, number // cuts), number % cuts
        index, is_aside = code // 2, code % 2
        shard = jnp.where(is_aside == 1, aside_shard(index // gps), main_shard(index // gps, skip))
        part_of = index % gps
        first = bit_flip(r, shard, R) * bpd + part_of * gb
        at = pl.ds(pl.multiple_of(part_of * group_rows, group_rows), group_rows)
        cols = pl.ds(pl.multiple_of(q * dot_cols, dot_cols), dot_cols)
        right = colp[shard, at, cols].astype(jnp.float32)
        left = rowp[shard, at, :]
        for e in range(ne):
            prod = jnp.dot(left, kern[e, :, cols], preferred_element_type=jnp.float32) * right
            thin = prod[:, :LANES]
            for k in range(1, dot_cols // LANES):
                thin = thin + prod[:, k * LANES:(k + 1) * LANES]
            total = sig[e]
            for b in range(gb):
                miss = jnp.full((8, LANES), freq[e] - energy[first + b], jnp.float32)
                weight = (1.0 / (1.0 + miss * miss))[:1]
                total = total + weight * thin[b * states:(b + 1) * states]
            sig[e] = total
        return carry

    pieces = len(plan.groups) * cuts

    def pieces_by(tick):
        ready = jnp.minimum(count(plan.row_need, tick - lag), count(plan.col_need, tick)) * cuts
        pace = jnp.maximum(PIECE_RATE * (tick - plan.build_ticks + 1), 0)
        return jnp.minimum(ready, pace)

    def at_most(value, most):
        return jnp.minimum(jnp.maximum(value, 0), most)

    def tick_step(tick, carry):
        if bits:
            paced = at_most(tick // 2 + 1, bpd)
            lax.fori_loop(jnp.where(is_heavy, at_most((tick + 1) // 2, bpd), jnp.where(tick == 0, 0, bpd)),
                          jnp.where(is_heavy, paced, bpd), send_near, 0)
        lax.fori_loop(count(plan.col_ticks, tick - 1), count(plan.col_ticks, tick), col_event, 0)

        @pl.when(at_home)
        def _():
            lax.fori_loop(count(plan.home_ticks, tick - 1), count(plan.home_ticks, tick), home_event, 0)

        @pl.when(jnp.logical_not(at_home))
        def _():
            since = tick - lag + 1
            lax.fori_loop(at_most(since - 1, plan.mains), at_most(since, plan.mains), main_event, 0)
            lax.fori_loop(count(plan.aside_ticks, tick - 1), count(plan.aside_ticks, tick), aside_event, 0)

        relay(tick)
        lax.fori_loop(at_most(BUILD_RATE * tick, blocks), at_most(BUILD_RATE * (tick + 1), blocks), make_block, 0)
        lax.fori_loop(pieces_by(tick - 1), pieces_by(tick), piece, 0)
        return carry
    ticks = plan.ticks
    while PIECE_RATE * (ticks - plan.build_ticks) < pieces:
        ticks += 1
    lax.fori_loop(0, ticks, tick_step, 0)

    for owner in range(Z):
        for e in range(ne):
            part[owner, e] = sig[e, owner * spc:(owner + 1) * spc]

    def s1_copy(d):
        return pltpu.make_async_remote_copy(
            src_ref=part.at[(z + d) % Z], dst_ref=recv1.at[d - 1],
            send_sem=s1_send.at[d - 1], recv_sem=s1_recv.at[d - 1], **dev(r, (z + d) % Z))

    def s2_copy(d, owner):
        return pltpu.make_async_remote_copy(
            src_ref=recv2.at[owner], dst_ref=recv2.at[owner],
            send_sem=s2_send.at[d - 1], recv_sem=s2_recv.at[owner], **dev((r + d) % R, z))

    for d in range(1, Z):
        s1_copy(d).start()

    for shard in range(1, R):
        low, high = shard & -shard, 1 << (shard.bit_length() - 1)

        def drain_col(b, carry, shard=shard, sems=0):
            col_copy(0, shard, b, partner, sems).wait_send()
            return carry
        if shard % 2 or low == high:
            lax.fori_loop(0, bpd, drain_col, 0)
        else:
            @pl.when(jnp.logical_not(backward(shard - high)))
            def _(drain_col=drain_col):
                lax.fori_loop(0, bpd, drain_col, 0)

            @pl.when(backward(shard - low))
            def _(drain_col=drain_col):
                lax.fori_loop(0, bpd, functools.partial(drain_col, sems=1), 0)

    def drain_rows(j, carry):
        m, b = j // bpd, j % bpd

        @pl.when(goes_up)
        def _():
            row_copy(main_shard(m, skip_up), b, up_send, upper).wait_send()

        @pl.when(goes_down)
        def _():
            row_copy(main_shard(m, skip_down), b, dn_send, lower).wait_send()
        return carry
    lax.fori_loop(0, plan.mains, drain_rows, 0)

    for d in range(Z):
        def drain_relay(i, carry, d=d):
            @pl.when(has_ahead)
            def _():
                hold_copy(d, i).wait_send()
            if d:
                give_copy(d, i, (panel_of(d) + Z) % Z).wait_send()
            return carry

        @pl.when(has_ahead if d == 0 else holds(d))
        def _():
            lax.fori_loop(0, plan.asides, drain_relay, 0)

    mine = part[z]
    for d in range(1, Z):
        s1_copy(d).wait_recv()
        mine = mine + recv1[d - 1]
    recv2[r] = mine
    for d in range(1, R):
        s2_copy(d, r).start()
    for d in range(1, R):
        s2_copy(d, (r + R - d) % R).wait_recv()
    full = recv2[0]
    for owner in range(1, R):
        full = full + recv2[owner]
    out[...] = jnp.sum(full, axis=-1)
    for d in range(1, Z):
        s1_copy(d).wait_send()
    for d in range(1, R):
        s2_copy(d, r).wait_send()


def solution(mesh):
    R, Z = mesh.shape["grow"], mesh.shape["gcol"]

    def shards(eps_static, eps_imag, frequency_grid, band_energy, pair_elements):
        height, breadth = eps_static.shape
        bpd, states, _ = pair_elements.shape
        ne = frequency_grid.shape[0]
        spc = states // Z
        rows = height // (4 * bpd)
        dma = pltpu.SemaphoreType.DMA
        units = R * bpd
        any_space = pl.BlockSpec(memory_space=pl.ANY)
        smem = pl.BlockSpec(memory_space=pltpu.SMEM)
        return pl.pallas_call(
            functools.partial(body, R, Z, bpd, states, height, breadth, ne),
            out_shape=jax.ShapeDtypeStruct((ne, spc), jnp.float32),
            in_specs=[smem, smem, any_space, any_space, any_space],
            out_specs=pl.BlockSpec(memory_space=pltpu.VMEM),
            scratch_shapes=[
                pltpu.VMEM((ne, height, breadth), jnp.bfloat16),
                pltpu.VMEM((R, bpd * states, breadth), jnp.bfloat16),
                pltpu.VMEM((R, bpd * states, height), jnp.bfloat16),
                pltpu.VMEM((2, rows, breadth), jnp.float32),
                pltpu.VMEM((2, rows, breadth), jnp.float32),
                pltpu.VMEM((ne, states, LANES), jnp.float32),
                pltpu.VMEM((Z, ne, spc, LANES), jnp.float32),
                pltpu.VMEM((max(Z - 1, 1), ne, spc, LANES), jnp.float32),
                pltpu.VMEM((R, ne, spc, LANES), jnp.float32),
                pltpu.VMEM((max(Z - 1, 1), R // Z * bpd * states, height), jnp.bfloat16),
                dma((2, 2)), dma, dma((2 * units,)), dma((units,)), dma((units,)),
                dma((units,)), dma((units,)),
                dma((Z,)), dma((Z,)), dma((R,)), dma((R,)),
                dma((R * bpd,)), dma((R * bpd,)), dma((R * bpd,)),
            ],
            compiler_params=pltpu.CompilerParams(
                collective_id=0, has_side_effects=True, vmem_limit_bytes=63 * 1024 * 1024),
            name="pole_sigma",
        )(frequency_grid, band_energy, eps_static, eps_imag,
          pair_elements.reshape(bpd * states, breadth))

    return jax.shard_map(
        shards,
        mesh=mesh,
        in_specs=(P("grow", "gcol"), P("grow", "gcol"), P(), P(), P("grow", None, "gcol")),
        out_specs=P(None, "gcol"),
        check_vma=False,
    )
```

```python
import functools

import jax
import jax.numpy as jnp
from jax import lax
from jax.experimental import pallas as pl
from jax.experimental.pallas import tpu as pltpu
from jax.sharding import PartitionSpec as P

LANES = 128
SUB_ROWS = 32
SUB_COLS = 512
DOT_ROWS = 128
DOT_COLS = 1536
EARLY_COLS = 512
EARLY_STEP = 1
EARLY_WAIT = 1
BUILD_RATE = 2
PIECE_RATE = (3, 2)
LEAD = 6
COL_START = 4
FAR_WAIT = 2
NEAR_STEP = 1
PASS_STEP = 2
PASS_EARLY = 2
END_START = 3
END_STEP = 5
END_BASE = -2
ASIDE_WAIT = 1
HOP_LAG = (3, 2)


def bit_flip(index, mask, extent):
    total, bit = 0, 1
    while bit < extent:
        total = total + ((index // bit + mask // bit) % 2) * bit
        bit *= 2
    return total


def flag(condition):
    return jnp.where(condition, 1, 0)


def count(table, tick):
    total = 0
    for entry in table:
        total = total + flag(tick >= entry)
    return total


def look(table, index):
    value = table[0]
    for n in range(1, len(table)):
        value = jnp.where(index >= n, table[n], value)
    return value


def rising(ticks):
    out = []
    for tick in ticks:
        out.append(max(tick, out[-1] if out else tick))
    return out


class Plan:
    def __init__(self, R, Z, bpd, states, height, breadth, blocks):
        ratio = R // Z
        self.mains, self.asides = (R - ratio) * bpd, ratio * bpd
        levels = {}
        for shard in range(R):
            levels.setdefault(bin(shard // 2).count("1"), []).append(shard)
        self.col_order, self.col_ticks = [], []
        tick = COL_START
        for level in sorted(levels):
            shards = sorted(levels[level], key=lambda shard: (shard % 2, shard))
            if level == 0:
                found = [b + bpd * shard for shard in shards for b in range(bpd)]
                ticks = [n // 4 for n in range(len(found))]
            else:
                found = [b + bpd * shard for b in range(bpd) for shard in shards]
                each = 2 if level == 1 else 1
                tick += FAR_WAIT if level == 2 else 0
                ticks = [tick + n // each for n in range(len(found))]
                tick = ticks[-1] + 1
            self.col_order += found
            self.col_ticks += ticks
        due = dict(zip(self.col_order, self.col_ticks))
        main_due = [due[j] if j < ratio * bpd else max(due[j], due[j + ratio * bpd]) for j in range(self.mains)]
        self.home_ticks = rising([max(0, j - LEAD, main_due[j]) for j in range(self.mains)])
        aside_due = [max(due[k + bpd * ratio * c] for c in range(1, Z)) for k in range(self.asides)]
        step = Z - 1
        self.relay_pass, self.relay_end = [], []
        for d in range(Z):
            self.relay_pass.append([PASS_STEP * d + i + (step - 1) * max(0, i - PASS_EARLY) for i in range(self.asides)])
            spread = [step * i + d + END_START for i in range(self.asides)]
            self.relay_end.append(rising([max(tick, END_STEP * d + END_BASE + 2 * i) for i, tick in enumerate(spread)]))
        self.aside_ticks = rising([max(t[k] for t in self.relay_end[1:]) + ASIDE_WAIT for k in range(self.asides)])
        self.near_ticks = [NEAR_STEP * b for b in range(bpd)]
        most = self.lag(Z - 1)
        self.gb = max(1, min(bpd, DOT_ROWS // states))
        self.gps = bpd // self.gb
        found = []
        for g in range(self.mains // self.gb):
            units = range(g * self.gb, (g + 1) * self.gb)
            found.append((units[-1], max(main_due[j] for j in units), 2 * g))
        for g in range(self.asides // self.gb):
            units = range(g * self.gb, (g + 1) * self.gb)
            found.append((0, max([self.aside_ticks[units[-1]]] + [aside_due[k] for k in units]), 2 * g + 1))
        found.sort(key=lambda entry: (max(entry[0] + self.lag(1), entry[1]), entry[0]))
        self.last = (2 * (self.mains // self.gb - 1), 2 * (self.asides // self.gb - 1) + 1)
        start = EARLY_WAIT + max(entry[1] for entry in found if entry[2] == self.last[0])
        start = max(start, EARLY_WAIT + max(aside_due))
        self.early_cols = min(EARLY_COLS, height)
        while height % self.early_cols:
            self.early_cols //= 2
        self.early_ticks = [start + EARLY_STEP * n for n in range(height // self.early_cols)]
        found = [entry for entry in found if entry[2] not in self.last]
        self.groups = [entry[2] for entry in found]
        self.row_need = rising([entry[0] for entry in found])
        self.col_need = rising([entry[1] for entry in found])
        self.ticks = 1 + max(self.mains + most, self.row_need[-1] + most, self.col_need[-1] + 1, self.aside_ticks[-1], self.early_ticks[-1],
                             max(t[-1] for t in self.relay_pass), max(t[-1] for t in self.relay_end))
        self.build_ticks = -(-blocks // BUILD_RATE)

    def lag(self, hops):
        return HOP_LAG[0] * hops // HOP_LAG[1]


def body(R, Z, bpd, states, height, breadth, ne,
         freq, energy, es_hbm, ei_hbm, pair_hbm, out,
         kern, colp, rowp, es_buf, ei_buf, sig, part, recv1, recv2, hold, early, stage,
         eps_sem, own_sem, col_send, col_recv, row_recv, up_send, dn_send,
         s1_send, s1_recv, s2_send, s2_recv, hold_send, hold_recv, give_send):
    r = lax.axis_index("grow")
    z = lax.axis_index("gcol")
    ratio = R // Z
    home = r // ratio
    core = r % ratio
    offset = pl.multiple_of(core * height, height)
    spc = states // Z
    units = R * bpd
    blocks = 4 * bpd
    rows = height // blocks
    plan = Plan(R, Z, bpd, states, height, breadth, blocks)

    def dev(row, col):
        return dict(device_id={"grow": row, "gcol": col}, device_id_type=pl.DeviceIdType.MESH)

    def eps_copies(block, slot):
        at = pl.multiple_of(block * rows, rows)
        return (pltpu.make_async_copy(es_hbm.at[pl.ds(at, rows), :], es_buf.at[slot], eps_sem.at[0, slot]),
                pltpu.make_async_copy(ei_hbm.at[pl.ds(at, rows), :], ei_buf.at[slot], eps_sem.at[1, slot]))

    own = pltpu.make_async_copy(pair_hbm, colp.at[0], own_sem)
    own.start()
    for copy in eps_copies(0, 0):
        copy.start()

    barrier = pltpu.get_barrier_semaphore()
    for d in range(1, R):
        pl.semaphore_signal(barrier, inc=1, **dev((r + d) % R, z))
    for d in range(1, Z):
        pl.semaphore_signal(barrier, inc=1, **dev(r, (z + d) % Z))
    sig[...] = jnp.zeros_like(sig)
    own.wait()
    pl.semaphore_wait(barrier, R + Z - 2)

    def unit_rows(b):
        return pl.ds(pl.multiple_of(b * states, states), states)

    def col_copy(src_shard, dst_shard, b, row, sems=0):
        return pltpu.make_async_remote_copy(
            src_ref=colp.at[src_shard, unit_rows(b), :], dst_ref=colp.at[dst_shard, unit_rows(b), :],
            send_sem=col_send.at[sems * units + dst_shard * bpd + b], recv_sem=col_recv.at[dst_shard * bpd + b],
            **dev(row, z))

    partner = bit_flip(r, 1, R)
    bits = []
    while 2 ** (len(bits) + 1) < R:
        bits.append(2 ** (len(bits) + 1))

    top = bits[-1] if bits else 1
    heavy = jnp.where(2 * z < Z, 0, Z - 1)
    is_heavy = home == heavy

    def backward(shard):
        source = bit_flip(r, shard, R)
        corner = jnp.logical_or(source // ratio == 0, source // ratio == Z - 1)
        return jnp.logical_or(corner, source // top % 2 == heavy * ratio // top % 2)

    def send_own(b, carry):
        for bit in [1] + bits[1:]:
            col_copy(0, bit, b, bit_flip(r, bit, R)).start()
        return carry
    lax.fori_loop(0, bpd, send_own, 0)

    def send_near(b, carry):
        col_copy(0, bits[0], b, bit_flip(r, bits[0], R)).start()
        return carry

    at_home = z == home
    goes_up = jnp.logical_and(z >= home, z < Z - 1)
    goes_down = jnp.logical_and(z <= home, z > 0)
    upper = (z + 1) % Z
    lower = (z + Z - 1) % Z
    hops = jnp.where(z > home, z - home, home - z)
    lag = plan.lag(hops)
    skip_up = bit_flip(home, Z - 1, Z) * ratio
    skip_down = home * ratio
    skip = jnp.where(at_home, R - ratio, jnp.where(z < home, skip_down, skip_up))

    def main_shard(m, skipped):
        return m + ratio * flag(m >= skipped)

    def aside_shard(a):
        return skip + a

    def row_copy(shard, b, sems, col):
        u = shard * bpd + b
        ref = rowp.at[shard, unit_rows(b), :]
        return pltpu.make_async_remote_copy(
            src_ref=ref, dst_ref=ref, send_sem=sems.at[u], recv_sem=row_recv.at[u], **dev(r, col))

    def home_copy(shard, b, sems, col):
        u = shard * bpd + b
        return pltpu.make_async_remote_copy(
            src_ref=colp.at[shard, unit_rows(b), pl.ds(offset, height)], dst_ref=rowp.at[shard, unit_rows(b), :],
            send_sem=sems.at[u], recv_sem=row_recv.at[u], **dev(r, col))

    def col_event(n, carry):
        u = look(plan.col_order, n)
        shard, b = u // bpd, u % bpd

        @pl.when(shard >= 1)
        def _():
            col_copy(0, shard, b, partner).wait_recv()

        @pl.when(jnp.logical_and(shard >= 2, shard % 2 == 0))
        def _():
            col_copy(shard, shard + 1, b, partner).start()
            for bit in bits[1:]:
                @pl.when(jnp.logical_and(shard < bit, jnp.logical_not(backward(shard))))
                def _(bit=bit):
                    col_copy(shard, shard + bit, b, bit_flip(r, bit, R)).start()
            for bit in bits[:-1]:
                @pl.when(jnp.logical_and(shard % (2 * bit) == 0, backward(shard)))
                def _(bit=bit):
                    col_copy(shard, shard + bit, b, bit_flip(r, bit, R), 1).start()

        @pl.when(at_home)
        def _():
            local = pltpu.make_async_copy(
                colp.at[shard, unit_rows(b), pl.ds(offset, height)],
                rowp.at[shard, unit_rows(b), :], row_recv.at[u])
            local.start()
            local.wait()
        return carry

    def home_event(j, carry):
        m, b = j // bpd, j % bpd

        @pl.when(goes_up)
        def _():
            home_copy(main_shard(m, skip_up), b, up_send, upper).start()

        @pl.when(goes_down)
        def _():
            home_copy(main_shard(m, skip_down), b, dn_send, lower).start()
        return carry

    def main_event(j, carry):
        shard, b = main_shard(j // bpd, skip), j % bpd
        row_copy(shard, b, up_send, upper).wait_recv()

        @pl.when(goes_up)
        def _():
            row_copy(shard, b, up_send, upper).start()

        @pl.when(goes_down)
        def _():
            row_copy(shard, b, dn_send, lower).start()
        return carry

    def aside_event(k, carry):
        row_copy(aside_shard(k // bpd), k % bpd, up_send, upper).wait_recv()
        return carry

    relay_down = home == 0
    relays = jnp.logical_or(relay_down, home == Z - 1)
    ahead = jnp.where(relay_down, z - 1, z + 1)
    has_ahead = jnp.logical_and(relays, jnp.logical_and(ahead >= 0, ahead < Z))
    ahead_col = (ahead + Z) % Z
    ends = jnp.logical_and(relays, jnp.logical_not(has_ahead))

    def hold_rows(i):
        return pl.ds(pl.multiple_of(i * states, states), states)

    def hold_copy(d, i):
        if d == 0:
            src = colp.at[i // bpd, unit_rows(i % bpd), pl.ds(offset, height)]
        else:
            src = hold.at[d - 1, hold_rows(i), :]
        return pltpu.make_async_remote_copy(
            src_ref=src, dst_ref=hold.at[min(d, Z - 2), hold_rows(i), :],
            send_sem=hold_send.at[d * plan.asides + i], recv_sem=hold_recv.at[min(d, Z - 2) * plan.asides + i],
            **dev(r, ahead_col))

    def give_copy(d, i, panel):
        to = panel * ratio + core
        shard = bit_flip(panel, home, Z) * ratio + i // bpd
        return pltpu.make_async_remote_copy(
            src_ref=hold.at[d - 1, hold_rows(i), :], dst_ref=rowp.at[shard, unit_rows(i % bpd), :],
            send_sem=give_send.at[(d - 1) * plan.asides + i], recv_sem=row_recv.at[shard * bpd + i % bpd],
            **dev(to, z))

    def panel_of(d):
        return jnp.where(relay_down, z + d, z - d)

    def holds(d):
        return jnp.logical_and(relays, jnp.logical_and(panel_of(d) >= 0, panel_of(d) < Z))

    def relay(tick):
        for d in range(Z):
            def item(i, carry, d=d):
                if d == 0:
                    hold_copy(d, i).start()
                    return carry
                hold_copy(d - 1, i).wait_recv()

                @pl.when(has_ahead)
                def _():
                    hold_copy(d, i).start()
                give_copy(d, i, (panel_of(d) + Z) % Z).start()
                return carry

            passing = (count(plan.relay_pass[d], tick - 1), count(plan.relay_pass[d], tick))
            if d == 0:
                live = has_ahead
                lo, hi = passing
            else:
                live = holds(d)
                lo = jnp.where(ends, count(plan.relay_end[d], tick - 1), passing[0])
                hi = jnp.where(ends, count(plan.relay_end[d], tick), passing[1])

            @pl.when(jnp.logical_and(live, hi > lo))
            def _():
                lax.fori_loop(lo, hi, item, 0)

    diagonal = r * height - z * breadth
    sub_rows = min(SUB_ROWS, rows)
    sub_cols = min(SUB_COLS, breadth)
    col_steps = breadth // sub_cols
    f0, f1, f2 = freq[0], freq[1], freq[2]

    def make_block(block, carry):
        slot = block % 2

        @pl.when(block + 1 < blocks)
        def _():
            for copy in eps_copies(block + 1, 1 - slot):
                copy.start()
        for copy in eps_copies(block, slot):
            copy.wait()
        base = pl.multiple_of(block * rows, rows)

        def chunk(n, carry):
            at_row = pl.multiple_of(n // col_steps * sub_rows, sub_rows)
            at_col = pl.multiple_of(n % col_steps * sub_cols, sub_cols)
            where = (pl.ds(at_row, sub_rows), pl.ds(at_col, sub_cols))
            gap = (lax.broadcasted_iota(jnp.int32, (sub_rows, sub_cols), 0)
                   - lax.broadcasted_iota(jnp.int32, (sub_rows, sub_cols), 1))
            one = jnp.where(gap == at_col - at_row - base - diagonal, 1.0, 0.0)
            static = es_buf[(slot,) + where] - one
            imag = ei_buf[(slot,) + where] - one
            spread = static - imag
            over = imag * imag + 0.25
            under = spread * spread + 0.25
            pole = over * lax.rsqrt(over * under)
            p0, p1, p2 = pole + f0, pole + f1, pole + f2
            p01 = p0 * p1
            scale = -static * pole / (p01 * p2)
            to = (pl.ds(pl.multiple_of(base + at_row, sub_rows), sub_rows), where[1])
            kern[(0,) + to] = (p1 * p2 * scale).astype(jnp.bfloat16)
            kern[(1,) + to] = (p0 * p2 * scale).astype(jnp.bfloat16)
            kern[(2,) + to] = (p01 * scale).astype(jnp.bfloat16)
            return carry
        lax.fori_loop(0, rows // sub_rows * col_steps, chunk, 0)
        return carry

    gb, gps = plan.gb, plan.gps
    group_rows = gb * states
    dot_cols = min(DOT_COLS, breadth)
    while breadth % dot_cols:
        dot_cols //= 2
    cuts = breadth // dot_cols

    def place(code):
        index, is_aside = code // 2, code % 2
        shard = jnp.where(is_aside == 1, aside_shard(index // gps), main_shard(index // gps, skip))
        part_of = index % gps
        first = bit_flip(r, shard, R) * bpd + part_of * gb
        return shard, pl.ds(pl.multiple_of(part_of * group_rows, group_rows), group_rows), first

    def gather_sum(e, prod, first):
        thin = prod[:, :LANES]
        for k in range(1, prod.shape[1] // LANES):
            thin = thin + prod[:, k * LANES:(k + 1) * LANES]
        total = sig[e]
        for b in range(gb):
            miss = jnp.full((8, LANES), freq[e] - energy[first + b], jnp.float32)
            weight = (1.0 / (1.0 + miss * miss))[:1]
            total = total + weight * thin[b * states:(b + 1) * states]
        sig[e] = total

    def piece(number, carry):
        q = number % cuts
        shard, at, first = place(look(plan.groups, number // cuts))
        cols = pl.ds(pl.multiple_of(q * dot_cols, dot_cols), dot_cols)
        right = colp[shard, at, cols].astype(jnp.float32)
        left = rowp[shard, at, :]
        for e in range(ne):
            gather_sum(e, jnp.dot(left, kern[e, :, cols], preferred_element_type=jnp.float32) * right, first)
        return carry

    def early_piece(n, carry):
        @pl.when(n == 0)
        def _():
            for half, code in enumerate(plan.last):
                shard, at, _ = place(code)

                def stage_rows(i, carry, half=half, shard=shard, at=at):
                    step = pl.ds(pl.multiple_of(i * 16, 16), 16)
                    to = pl.ds(pl.multiple_of(half * group_rows + i * 16, 16), 16)
                    from_rows = pl.ds(pl.multiple_of(at.start + i * 16, 16), 16)
                    stage[to, :] = colp[shard, from_rows, :]
                    return carry
                lax.fori_loop(0, group_rows // 16, stage_rows, 0)
        some = pl.ds(pl.multiple_of(n * plan.early_cols, plan.early_cols), plan.early_cols)
        left = stage[...]
        for e in range(ne):
            early[e, :, some] = lax.dot_general(
                left, kern[e, some, :], (((1,), (1,)), ((), ())), preferred_element_type=jnp.float32).astype(jnp.bfloat16)
        return carry

    def finish():
        for half, code in enumerate(plan.last):
            shard, at, first = place(code)
            right = rowp[shard, at, :].astype(jnp.float32)
            for e in range(ne):
                left = early[e, half * group_rows:(half + 1) * group_rows, :].astype(jnp.float32)
                gather_sum(e, left * right, first)

    pieces = len(plan.groups) * cuts

    def pieces_by(tick):
        ready = jnp.minimum(count(plan.row_need, tick - lag), count(plan.col_need, tick)) * cuts
        pace = PIECE_RATE[0] * jnp.maximum(tick - plan.build_ticks + 1, 0) // PIECE_RATE[1]
        return jnp.minimum(ready, pace)

    def at_most(value, most):
        return jnp.minimum(jnp.maximum(value, 0), most)

    def tick_step(tick, carry):
        if bits:
            lax.fori_loop(jnp.where(is_heavy, count(plan.near_ticks, tick - 1), bpd * flag(tick > 0)),
                          jnp.where(is_heavy, count(plan.near_ticks, tick), bpd), send_near, 0)
        lax.fori_loop(count(plan.col_ticks, tick - 1), count(plan.col_ticks, tick), col_event, 0)

        @pl.when(at_home)
        def _():
            lax.fori_loop(count(plan.home_ticks, tick - 1), count(plan.home_ticks, tick), home_event, 0)

        @pl.when(jnp.logical_not(at_home))
        def _():
            since = tick - lag + 1
            lax.fori_loop(at_most(since - 1, plan.mains), at_most(since, plan.mains), main_event, 0)
            lax.fori_loop(count(plan.aside_ticks, tick - 1), count(plan.aside_ticks, tick), aside_event, 0)

        relay(tick)
        lax.fori_loop(at_most(BUILD_RATE * tick, blocks), at_most(BUILD_RATE * (tick + 1), blocks), make_block, 0)
        lax.fori_loop(pieces_by(tick - 1), pieces_by(tick), piece, 0)
        lax.fori_loop(count(plan.early_ticks, tick - 1), count(plan.early_ticks, tick), early_piece, 0)
        return carry
    ticks = plan.ticks
    while PIECE_RATE[0] * (ticks - plan.build_ticks) // PIECE_RATE[1] < pieces:
        ticks += 1
    lax.fori_loop(0, ticks, tick_step, 0)
    finish()

    for owner in range(Z):
        for e in range(ne):
            part[owner, e] = sig[e, owner * spc:(owner + 1) * spc]

    def s1_copy(d):
        return pltpu.make_async_remote_copy(
            src_ref=part.at[(z + d) % Z], dst_ref=recv1.at[d - 1],
            send_sem=s1_send.at[d - 1], recv_sem=s1_recv.at[d - 1], **dev(r, (z + d) % Z))

    def s2_copy(d, owner):
        return pltpu.make_async_remote_copy(
            src_ref=recv2.at[owner], dst_ref=recv2.at[owner],
            send_sem=s2_send.at[d - 1], recv_sem=s2_recv.at[owner], **dev((r + d) % R, z))

    for d in range(1, Z):
        s1_copy(d).start()

    for shard in range(1, R):
        low, high = shard & -shard, 1 << (shard.bit_length() - 1)

        def drain_col(b, carry, shard=shard, sems=0):
            col_copy(0, shard, b, partner, sems).wait_send()
            return carry
        if shard % 2 or low == high:
            lax.fori_loop(0, bpd, drain_col, 0)
        else:
            @pl.when(jnp.logical_not(backward(shard - high)))
            def _(drain_col=drain_col):
                lax.fori_loop(0, bpd, drain_col, 0)

            @pl.when(backward(shard - low))
            def _(drain_col=drain_col):
                lax.fori_loop(0, bpd, functools.partial(drain_col, sems=1), 0)

    def drain_rows(j, carry):
        m, b = j // bpd, j % bpd

        @pl.when(goes_up)
        def _():
            row_copy(main_shard(m, skip_up), b, up_send, upper).wait_send()

        @pl.when(goes_down)
        def _():
            row_copy(main_shard(m, skip_down), b, dn_send, lower).wait_send()
        return carry
    lax.fori_loop(0, plan.mains, drain_rows, 0)

    for d in range(Z):
        def drain_relay(i, carry, d=d):
            @pl.when(has_ahead)
            def _():
                hold_copy(d, i).wait_send()
            if d:
                give_copy(d, i, (panel_of(d) + Z) % Z).wait_send()
            return carry

        @pl.when(has_ahead if d == 0 else holds(d))
        def _():
            lax.fori_loop(0, plan.asides, drain_relay, 0)

    mine = part[z]
    for d in range(1, Z):
        s1_copy(d).wait_recv()
        mine = mine + recv1[d - 1]
    recv2[r] = mine
    for d in range(1, R):
        s2_copy(d, r).start()
    for d in range(1, R):
        s2_copy(d, (r + R - d) % R).wait_recv()
    full = recv2[0]
    for owner in range(1, R):
        full = full + recv2[owner]
    out[...] = jnp.sum(full, axis=-1)
    for d in range(1, Z):
        s1_copy(d).wait_send()
    for d in range(1, R):
        s2_copy(d, r).wait_send()


def solution(mesh):
    R, Z = mesh.shape["grow"], mesh.shape["gcol"]

    def shards(eps_static, eps_imag, frequency_grid, band_energy, pair_elements):
        height, breadth = eps_static.shape
        bpd, states, _ = pair_elements.shape
        ne = frequency_grid.shape[0]
        spc = states // Z
        rows = height // (4 * bpd)
        dma = pltpu.SemaphoreType.DMA
        units = R * bpd
        pair_rows = 2 * states * max(1, min(bpd, DOT_ROWS // states))
        any_space = pl.BlockSpec(memory_space=pl.ANY)
        smem = pl.BlockSpec(memory_space=pltpu.SMEM)
        return pl.pallas_call(
            functools.partial(body, R, Z, bpd, states, height, breadth, ne),
            out_shape=jax.ShapeDtypeStruct((ne, spc), jnp.float32),
            in_specs=[smem, smem, any_space, any_space, any_space],
            out_specs=pl.BlockSpec(memory_space=pltpu.VMEM),
            scratch_shapes=[
                pltpu.VMEM((ne, height, breadth), jnp.bfloat16),
                pltpu.VMEM((R, bpd * states, breadth), jnp.bfloat16),
                pltpu.VMEM((R, bpd * states, height), jnp.bfloat16),
                pltpu.VMEM((2, rows, breadth), jnp.float32),
                pltpu.VMEM((2, rows, breadth), jnp.float32),
                pltpu.VMEM((ne, states, LANES), jnp.float32),
                pltpu.VMEM((Z, ne, spc, LANES), jnp.float32),
                pltpu.VMEM((max(Z - 1, 1), ne, spc, LANES), jnp.float32),
                pltpu.VMEM((R, ne, spc, LANES), jnp.float32),
                pltpu.VMEM((max(Z - 1, 1), R // Z * bpd * states, height), jnp.bfloat16),
                pltpu.VMEM((ne, pair_rows, height), jnp.bfloat16),
                pltpu.VMEM((pair_rows, breadth), jnp.bfloat16),
                dma((2, 2)), dma, dma((2 * units,)), dma((units,)), dma((units,)),
                dma((units,)), dma((units,)),
                dma((Z,)), dma((Z,)), dma((R,)), dma((R,)),
                dma((R * bpd,)), dma((R * bpd,)), dma((R * bpd,)),
            ],
            compiler_params=pltpu.CompilerParams(
                collective_id=0, has_side_effects=True, vmem_limit_bytes=63 * 1024 * 1024 + 512 * 1024),
            name="pole_sigma",
        )(frequency_grid, band_energy, eps_static, eps_imag,
          pair_elements.reshape(bpd * states, breadth))

    return jax.shard_map(
        shards,
        mesh=mesh,
        in_specs=(P("grow", "gcol"), P("grow", "gcol"), P(), P(), P("grow", None, "gcol")),
        out_specs=P(None, "gcol"),
        check_vma=False,
    )
```

```python
import functools

import jax
import jax.numpy as jnp
from jax import lax
from jax.experimental import pallas as pl
from jax.experimental.pallas import tpu as pltpu
from jax.sharding import PartitionSpec as P

LANES = 128
SUB_ROWS = 32
SUB_COLS = 1536
DOT_ROWS = 128
DOT_COLS = 1536
EARLY_COLS = 512
EARLY_STEP = 1
EARLY_WAIT = 1
BUILD_RATE = 2
PIECE_RATE = (3, 2)
LEAD = 6
COL_START = 4
FAR_WAIT = 2
NEAR_STEP = 1
PASS_STEP = 2
PASS_EARLY = 2
END_START = 3
END_STEP = 5
END_BASE = -2
ASIDE_WAIT = 1
HOP_LAG = (3, 2)


def bit_flip(index, mask, extent):
    total, bit = 0, 1
    while bit < extent:
        total = total + ((index // bit + mask // bit) % 2) * bit
        bit *= 2
    return total


def flag(condition):
    return jnp.where(condition, 1, 0)


def count(table, tick):
    total = 0
    for entry in table:
        total = total + flag(tick >= entry)
    return total


def look(table, index):
    value = table[0]
    for n in range(1, len(table)):
        value = jnp.where(index >= n, table[n], value)
    return value


def rising(ticks):
    out = []
    for tick in ticks:
        out.append(max(tick, out[-1] if out else tick))
    return out


class Plan:
    def __init__(self, R, Z, bpd, states, height, breadth, blocks):
        ratio = R // Z
        self.mains, self.asides = (R - ratio) * bpd, ratio * bpd
        levels = {}
        for shard in range(R):
            levels.setdefault(bin(shard // 2).count("1"), []).append(shard)
        self.col_order, self.col_ticks = [], []
        tick = COL_START
        for level in sorted(levels):
            shards = sorted(levels[level], key=lambda shard: (shard % 2, shard))
            if level == 0:
                found = [b + bpd * shard for shard in shards for b in range(bpd)]
                ticks = [n // 4 for n in range(len(found))]
            else:
                found = [b + bpd * shard for b in range(bpd) for shard in shards]
                each = 2 if level == 1 else 1
                tick += FAR_WAIT if level == 2 else 0
                ticks = [tick + n // each for n in range(len(found))]
                tick = ticks[-1] + 1
            self.col_order += found
            self.col_ticks += ticks
        due = dict(zip(self.col_order, self.col_ticks))
        main_due = [due[j] if j < ratio * bpd else max(due[j], due[j + ratio * bpd]) for j in range(self.mains)]
        self.home_ticks = rising([max(0, j - LEAD, main_due[j]) for j in range(self.mains)])
        aside_due = [max(due[k + bpd * ratio * c] for c in range(1, Z)) for k in range(self.asides)]
        step = Z - 1
        self.relay_pass, self.relay_end = [], []
        for d in range(Z):
            self.relay_pass.append([PASS_STEP * d + i + (step - 1) * max(0, i - PASS_EARLY) for i in range(self.asides)])
            spread = [step * i + d + END_START for i in range(self.asides)]
            self.relay_end.append(rising([max(tick, END_STEP * d + END_BASE + 2 * i) for i, tick in enumerate(spread)]))
        self.aside_ticks = rising([max(t[k] for t in self.relay_end[1:]) + ASIDE_WAIT for k in range(self.asides)])
        self.near_ticks = [NEAR_STEP * b for b in range(bpd)]
        most = self.lag(Z - 1)
        self.gb = max(1, min(bpd, DOT_ROWS // states))
        self.gps = bpd // self.gb
        found = []
        for g in range(self.mains // self.gb):
            units = range(g * self.gb, (g + 1) * self.gb)
            found.append((units[-1], max(main_due[j] for j in units), 2 * g))
        for g in range(self.asides // self.gb):
            units = range(g * self.gb, (g + 1) * self.gb)
            found.append((0, max([self.aside_ticks[units[-1]]] + [aside_due[k] for k in units]), 2 * g + 1))
        found.sort(key=lambda entry: (max(entry[0] + self.lag(1), entry[1]), entry[0]))
        self.last = (2 * (self.mains // self.gb - 1), 2 * (self.asides // self.gb - 1) + 1)
        start = EARLY_WAIT + max(entry[1] for entry in found if entry[2] == self.last[0])
        start = max(start, EARLY_WAIT + max(aside_due))
        self.early_cols = min(EARLY_COLS, height)
        while height % self.early_cols:
            self.early_cols //= 2
        self.early_ticks = [start + EARLY_STEP * n for n in range(height // self.early_cols)]
        found = [entry for entry in found if entry[2] not in self.last]
        self.groups = [entry[2] for entry in found]
        self.row_need = rising([entry[0] for entry in found])
        self.col_need = rising([entry[1] for entry in found])
        self.ticks = 1 + max(self.mains + most, self.row_need[-1] + most, self.col_need[-1] + 1, self.aside_ticks[-1], self.early_ticks[-1],
                             max(t[-1] for t in self.relay_pass), max(t[-1] for t in self.relay_end))
        self.build_ticks = -(-blocks // BUILD_RATE)

    def lag(self, hops):
        return HOP_LAG[0] * hops // HOP_LAG[1]


def body(R, Z, bpd, states, height, breadth, ne,
         freq, energy, es_hbm, ei_hbm, pair_hbm, out,
         kern, colp, rowp, es_buf, ei_buf, sig, part, recv1, recv2, hold, early, stage,
         eps_sem, own_sem, col_send, col_recv, row_recv, up_send, dn_send,
         s1_send, s1_recv, s2_send, s2_recv, hold_send, hold_recv, give_send):
    r = lax.axis_index("grow")
    z = lax.axis_index("gcol")
    ratio = R // Z
    home = r // ratio
    core = r % ratio
    offset = pl.multiple_of(core * height, height)
    spc = states // Z
    units = R * bpd
    blocks = 4 * bpd
    rows = height // blocks
    plan = Plan(R, Z, bpd, states, height, breadth, blocks)

    def dev(row, col):
        return dict(device_id={"grow": row, "gcol": col}, device_id_type=pl.DeviceIdType.MESH)

    def eps_copies(block, slot):
        at = pl.multiple_of(block * rows, rows)
        return (pltpu.make_async_copy(es_hbm.at[pl.ds(at, rows), :], es_buf.at[slot], eps_sem.at[0, slot]),
                pltpu.make_async_copy(ei_hbm.at[pl.ds(at, rows), :], ei_buf.at[slot], eps_sem.at[1, slot]))

    own = pltpu.make_async_copy(pair_hbm, colp.at[0], own_sem)
    own.start()
    for copy in eps_copies(0, 0):
        copy.start()

    barrier = pltpu.get_barrier_semaphore()
    for d in range(1, R):
        pl.semaphore_signal(barrier, inc=1, **dev((r + d) % R, z))
    for d in range(1, Z):
        pl.semaphore_signal(barrier, inc=1, **dev(r, (z + d) % Z))
    sig[...] = jnp.zeros_like(sig)
    own.wait()
    pl.semaphore_wait(barrier, R + Z - 2)

    def unit_rows(b):
        return pl.ds(pl.multiple_of(b * states, states), states)

    def col_copy(src_shard, dst_shard, b, row, sems=0):
        return pltpu.make_async_remote_copy(
            src_ref=colp.at[src_shard, unit_rows(b), :], dst_ref=colp.at[dst_shard, unit_rows(b), :],
            send_sem=col_send.at[sems * units + dst_shard * bpd + b], recv_sem=col_recv.at[dst_shard * bpd + b],
            **dev(row, z))

    partner = bit_flip(r, 1, R)
    bits = []
    while 2 ** (len(bits) + 1) < R:
        bits.append(2 ** (len(bits) + 1))

    top = bits[-1] if bits else 1
    heavy = jnp.where(2 * z < Z, 0, Z - 1)
    is_heavy = home == heavy

    def backward(shard):
        source = bit_flip(r, shard, R)
        corner = jnp.logical_or(source // ratio == 0, source // ratio == Z - 1)
        return jnp.logical_or(corner, source // top % 2 == heavy * ratio // top % 2)

    def send_own(b, carry):
        for bit in [1] + bits[1:]:
            col_copy(0, bit, b, bit_flip(r, bit, R)).start()
        return carry
    lax.fori_loop(0, bpd, send_own, 0)

    def send_near(b, carry):
        col_copy(0, bits[0], b, bit_flip(r, bits[0], R)).start()
        return carry

    at_home = z == home
    goes_up = jnp.logical_and(z >= home, z < Z - 1)
    goes_down = jnp.logical_and(z <= home, z > 0)
    upper = (z + 1) % Z
    lower = (z + Z - 1) % Z
    hops = jnp.where(z > home, z - home, home - z)
    lag = plan.lag(hops)
    skip_up = bit_flip(home, Z - 1, Z) * ratio
    skip_down = home * ratio
    skip = jnp.where(at_home, R - ratio, jnp.where(z < home, skip_down, skip_up))

    def main_shard(m, skipped):
        return m + ratio * flag(m >= skipped)

    def aside_shard(a):
        return skip + a

    def row_copy(shard, b, sems, col):
        u = shard * bpd + b
        ref = rowp.at[shard, unit_rows(b), :]
        return pltpu.make_async_remote_copy(
            src_ref=ref, dst_ref=ref, send_sem=sems.at[u], recv_sem=row_recv.at[u], **dev(r, col))

    def home_copy(shard, b, sems, col):
        u = shard * bpd + b
        return pltpu.make_async_remote_copy(
            src_ref=colp.at[shard, unit_rows(b), pl.ds(offset, height)], dst_ref=rowp.at[shard, unit_rows(b), :],
            send_sem=sems.at[u], recv_sem=row_recv.at[u], **dev(r, col))

    def col_event(n, carry):
        u = look(plan.col_order, n)
        shard, b = u // bpd, u % bpd

        @pl.when(shard >= 1)
        def _():
            col_copy(0, shard, b, partner).wait_recv()

        @pl.when(jnp.logical_and(shard >= 2, shard % 2 == 0))
        def _():
            col_copy(shard, shard + 1, b, partner).start()
            for bit in bits[1:]:
                @pl.when(jnp.logical_and(shard < bit, jnp.logical_not(backward(shard))))
                def _(bit=bit):
                    col_copy(shard, shard + bit, b, bit_flip(r, bit, R)).start()
            for bit in bits[:-1]:
                @pl.when(jnp.logical_and(shard % (2 * bit) == 0, backward(shard)))
                def _(bit=bit):
                    col_copy(shard, shard + bit, b, bit_flip(r, bit, R), 1).start()

        @pl.when(at_home)
        def _():
            local = pltpu.make_async_copy(
                colp.at[shard, unit_rows(b), pl.ds(offset, height)],
                rowp.at[shard, unit_rows(b), :], row_recv.at[u])
            local.start()
            local.wait()
        return carry

    def home_event(j, carry):
        m, b = j // bpd, j % bpd

        @pl.when(goes_up)
        def _():
            home_copy(main_shard(m, skip_up), b, up_send, upper).start()

        @pl.when(goes_down)
        def _():
            home_copy(main_shard(m, skip_down), b, dn_send, lower).start()
        return carry

    def main_event(j, carry):
        shard, b = main_shard(j // bpd, skip), j % bpd
        row_copy(shard, b, up_send, upper).wait_recv()

        @pl.when(goes_up)
        def _():
            row_copy(shard, b, up_send, upper).start()

        @pl.when(goes_down)
        def _():
            row_copy(shard, b, dn_send, lower).start()
        return carry

    def aside_event(k, carry):
        row_copy(aside_shard(k // bpd), k % bpd, up_send, upper).wait_recv()
        return carry

    relay_down = home == 0
    relays = jnp.logical_or(relay_down, home == Z - 1)
    ahead = jnp.where(relay_down, z - 1, z + 1)
    has_ahead = jnp.logical_and(relays, jnp.logical_and(ahead >= 0, ahead < Z))
    ahead_col = (ahead + Z) % Z
    ends = jnp.logical_and(relays, jnp.logical_not(has_ahead))

    def hold_rows(i):
        return pl.ds(pl.multiple_of(i * states, states), states)

    def hold_copy(d, i):
        if d == 0:
            src = colp.at[i // bpd, unit_rows(i % bpd), pl.ds(offset, height)]
        else:
            src = hold.at[d - 1, hold_rows(i), :]
        return pltpu.make_async_remote_copy(
            src_ref=src, dst_ref=hold.at[min(d, Z - 2), hold_rows(i), :],
            send_sem=hold_send.at[d * plan.asides + i], recv_sem=hold_recv.at[min(d, Z - 2) * plan.asides + i],
            **dev(r, ahead_col))

    def give_copy(d, i, panel):
        to = panel * ratio + core
        shard = bit_flip(panel, home, Z) * ratio + i // bpd
        return pltpu.make_async_remote_copy(
            src_ref=hold.at[d - 1, hold_rows(i), :], dst_ref=rowp.at[shard, unit_rows(i % bpd), :],
            send_sem=give_send.at[(d - 1) * plan.asides + i], recv_sem=row_recv.at[shard * bpd + i % bpd],
            **dev(to, z))

    def panel_of(d):
        return jnp.where(relay_down, z + d, z - d)

    def holds(d):
        return jnp.logical_and(relays, jnp.logical_and(panel_of(d) >= 0, panel_of(d) < Z))

    def relay(tick):
        for d in range(Z):
            def item(i, carry, d=d):
                if d == 0:
                    hold_copy(d, i).start()
                    return carry
                hold_copy(d - 1, i).wait_recv()

                @pl.when(has_ahead)
                def _():
                    hold_copy(d, i).start()
                give_copy(d, i, (panel_of(d) + Z) % Z).start()
                return carry

            passing = (count(plan.relay_pass[d], tick - 1), count(plan.relay_pass[d], tick))
            if d == 0:
                live = has_ahead
                lo, hi = passing
            else:
                live = holds(d)
                lo = jnp.where(ends, count(plan.relay_end[d], tick - 1), passing[0])
                hi = jnp.where(ends, count(plan.relay_end[d], tick), passing[1])

            @pl.when(jnp.logical_and(live, hi > lo))
            def _():
                lax.fori_loop(lo, hi, item, 0)

    diagonal = r * height - z * breadth
    sub_rows = min(SUB_ROWS, rows)
    sub_cols = min(SUB_COLS, breadth)
    col_steps = breadth // sub_cols
    f0, f1, f2 = freq[0], freq[1], freq[2]

    def make_block(block, carry):
        slot = block % 2

        @pl.when(block + 1 < blocks)
        def _():
            for copy in eps_copies(block + 1, 1 - slot):
                copy.start()
        for copy in eps_copies(block, slot):
            copy.wait()
        base = pl.multiple_of(block * rows, rows)

        def chunk(n, carry):
            at_row = pl.multiple_of(n // col_steps * sub_rows, sub_rows)
            at_col = pl.multiple_of(n % col_steps * sub_cols, sub_cols)
            where = (pl.ds(at_row, sub_rows), pl.ds(at_col, sub_cols))
            gap = (lax.broadcasted_iota(jnp.int32, (sub_rows, sub_cols), 0)
                   - lax.broadcasted_iota(jnp.int32, (sub_rows, sub_cols), 1))
            one = jnp.where(gap == at_col - at_row - base - diagonal, 1.0, 0.0)
            static = es_buf[(slot,) + where] - one
            imag = ei_buf[(slot,) + where] - one
            spread = static - imag
            over = imag * imag + 0.25
            under = spread * spread + 0.25
            pole = over * lax.rsqrt(over * under)
            p0, p1, p2 = pole + f0, pole + f1, pole + f2
            p01 = p0 * p1
            scale = -static * pole / (p01 * p2)
            to = (pl.ds(pl.multiple_of(base + at_row, sub_rows), sub_rows), where[1])
            kern[(0,) + to] = (p1 * p2 * scale).astype(jnp.bfloat16)
            kern[(1,) + to] = (p0 * p2 * scale).astype(jnp.bfloat16)
            kern[(2,) + to] = (p01 * scale).astype(jnp.bfloat16)
            return carry
        lax.fori_loop(0, rows // sub_rows * col_steps, chunk, 0)
        return carry

    gb, gps = plan.gb, plan.gps
    group_rows = gb * states
    dot_cols = min(DOT_COLS, breadth)
    while breadth % dot_cols:
        dot_cols //= 2
    cuts = breadth // dot_cols

    def place(code):
        index, is_aside = code // 2, code % 2
        shard = jnp.where(is_aside == 1, aside_shard(index // gps), main_shard(index // gps, skip))
        part_of = index % gps
        first = bit_flip(r, shard, R) * bpd + part_of * gb
        return shard, pl.ds(pl.multiple_of(part_of * group_rows, group_rows), group_rows), first

    def gather_sum(e, prod, first):
        thin = prod[:, :LANES]
        for k in range(1, prod.shape[1] // LANES):
            thin = thin + prod[:, k * LANES:(k + 1) * LANES]
        total = sig[e]
        for b in range(gb):
            miss = jnp.full((8, LANES), freq[e] - energy[first + b], jnp.float32)
            weight = (1.0 / (1.0 + miss * miss))[:1]
            total = total + weight * thin[b * states:(b + 1) * states]
        sig[e] = total

    def piece(number, carry):
        q = number % cuts
        shard, at, first = place(look(plan.groups, number // cuts))
        cols = pl.ds(pl.multiple_of(q * dot_cols, dot_cols), dot_cols)
        right = colp[shard, at, cols].astype(jnp.float32)
        left = rowp[shard, at, :]
        for e in range(ne):
            gather_sum(e, jnp.dot(left, kern[e, :, cols], preferred_element_type=jnp.float32) * right, first)
        return carry

    def early_piece(n, carry):
        @pl.when(n == 0)
        def _():
            for half, code in enumerate(plan.last):
                shard, at, _ = place(code)

                def stage_rows(i, carry, half=half, shard=shard, at=at):
                    step = pl.ds(pl.multiple_of(i * 16, 16), 16)
                    to = pl.ds(pl.multiple_of(half * group_rows + i * 16, 16), 16)
                    from_rows = pl.ds(pl.multiple_of(at.start + i * 16, 16), 16)
                    stage[to, :] = colp[shard, from_rows, :]
                    return carry
                lax.fori_loop(0, group_rows // 16, stage_rows, 0)
        some = pl.ds(pl.multiple_of(n * plan.early_cols, plan.early_cols), plan.early_cols)
        left = stage[...]
        for e in range(ne):
            early[e, :, some] = lax.dot_general(
                left, kern[e, some, :], (((1,), (1,)), ((), ())), preferred_element_type=jnp.float32).astype(jnp.bfloat16)
        return carry

    def finish():
        for half, code in enumerate(plan.last):
            shard, at, first = place(code)
            right = rowp[shard, at, :].astype(jnp.float32)
            for e in range(ne):
                left = early[e, half * group_rows:(half + 1) * group_rows, :].astype(jnp.float32)
                gather_sum(e, left * right, first)

    pieces = len(plan.groups) * cuts

    def pieces_by(tick):
        ready = jnp.minimum(count(plan.row_need, tick - lag), count(plan.col_need, tick)) * cuts
        pace = PIECE_RATE[0] * jnp.maximum(tick - plan.build_ticks + 1, 0) // PIECE_RATE[1]
        return jnp.minimum(ready, pace)

    def at_most(value, most):
        return jnp.minimum(jnp.maximum(value, 0), most)

    def tick_step(tick, carry):
        if bits:
            lax.fori_loop(jnp.where(is_heavy, count(plan.near_ticks, tick - 1), bpd * flag(tick > 0)),
                          jnp.where(is_heavy, count(plan.near_ticks, tick), bpd), send_near, 0)
        lax.fori_loop(count(plan.col_ticks, tick - 1), count(plan.col_ticks, tick), col_event, 0)

        @pl.when(at_home)
        def _():
            lax.fori_loop(count(plan.home_ticks, tick - 1), count(plan.home_ticks, tick), home_event, 0)

        @pl.when(jnp.logical_not(at_home))
        def _():
            since = tick - lag + 1
            lax.fori_loop(at_most(since - 1, plan.mains), at_most(since, plan.mains), main_event, 0)
            lax.fori_loop(count(plan.aside_ticks, tick - 1), count(plan.aside_ticks, tick), aside_event, 0)

        relay(tick)
        lax.fori_loop(at_most(BUILD_RATE * tick, blocks), at_most(BUILD_RATE * (tick + 1), blocks), make_block, 0)
        lax.fori_loop(pieces_by(tick - 1), pieces_by(tick), piece, 0)
        lax.fori_loop(count(plan.early_ticks, tick - 1), count(plan.early_ticks, tick), early_piece, 0)
        return carry
    ticks = plan.ticks
    while PIECE_RATE[0] * (ticks - plan.build_ticks) // PIECE_RATE[1] < pieces:
        ticks += 1
    lax.fori_loop(0, ticks, tick_step, 0)
    finish()

    part[...] = jnp.zeros_like(part)
    for owner in range(Z):
        part[owner, :ne, :spc] = jnp.sum(sig[:, owner * spc:(owner + 1) * spc, :], axis=-1)

    def s1_copy(d):
        return pltpu.make_async_remote_copy(
            src_ref=part.at[(z + d) % Z], dst_ref=recv1.at[d - 1],
            send_sem=s1_send.at[d - 1], recv_sem=s1_recv.at[d - 1], **dev(r, (z + d) % Z))

    def s2_copy(d, owner):
        return pltpu.make_async_remote_copy(
            src_ref=recv2.at[owner], dst_ref=recv2.at[owner],
            send_sem=s2_send.at[d - 1], recv_sem=s2_recv.at[owner], **dev((r + d) % R, z))

    for d in range(1, Z):
        s1_copy(d).start()

    for shard in range(1, R):
        low, high = shard & -shard, 1 << (shard.bit_length() - 1)

        def drain_col(b, carry, shard=shard, sems=0):
            col_copy(0, shard, b, partner, sems).wait_send()
            return carry
        if shard % 2 or low == high:
            lax.fori_loop(0, bpd, drain_col, 0)
        else:
            @pl.when(jnp.logical_not(backward(shard - high)))
            def _(drain_col=drain_col):
                lax.fori_loop(0, bpd, drain_col, 0)

            @pl.when(backward(shard - low))
            def _(drain_col=drain_col):
                lax.fori_loop(0, bpd, functools.partial(drain_col, sems=1), 0)

    def drain_rows(j, carry):
        m, b = j // bpd, j % bpd

        @pl.when(goes_up)
        def _():
            row_copy(main_shard(m, skip_up), b, up_send, upper).wait_send()

        @pl.when(goes_down)
        def _():
            row_copy(main_shard(m, skip_down), b, dn_send, lower).wait_send()
        return carry
    lax.fori_loop(0, plan.mains, drain_rows, 0)

    for d in range(Z):
        def drain_relay(i, carry, d=d):
            @pl.when(has_ahead)
            def _():
                hold_copy(d, i).wait_send()
            if d:
                give_copy(d, i, (panel_of(d) + Z) % Z).wait_send()
            return carry

        @pl.when(has_ahead if d == 0 else holds(d))
        def _():
            lax.fori_loop(0, plan.asides, drain_relay, 0)

    mine = part[z]
    for d in range(1, Z):
        s1_copy(d).wait_recv()
        mine = mine + recv1[d - 1]
    recv2[r] = mine
    for d in range(1, R):
        s2_copy(d, r).start()
    for d in range(1, R):
        s2_copy(d, (r + R - d) % R).wait_recv()
    full = recv2[0]
    for owner in range(1, R):
        full = full + recv2[owner]
    out[...] = full[:ne, :spc]
    for d in range(1, Z):
        s1_copy(d).wait_send()
    for d in range(1, R):
        s2_copy(d, r).wait_send()


def solution(mesh):
    R, Z = mesh.shape["grow"], mesh.shape["gcol"]

    def shards(eps_static, eps_imag, frequency_grid, band_energy, pair_elements):
        height, breadth = eps_static.shape
        bpd, states, _ = pair_elements.shape
        ne = frequency_grid.shape[0]
        spc = states // Z
        flat, wide = -(-ne // 8) * 8, -(-spc // LANES) * LANES
        rows = height // (4 * bpd)
        dma = pltpu.SemaphoreType.DMA
        units = R * bpd
        pair_rows = 2 * states * max(1, min(bpd, DOT_ROWS // states))
        any_space = pl.BlockSpec(memory_space=pl.ANY)
        smem = pl.BlockSpec(memory_space=pltpu.SMEM)
        return pl.pallas_call(
            functools.partial(body, R, Z, bpd, states, height, breadth, ne),
            out_shape=jax.ShapeDtypeStruct((ne, spc), jnp.float32),
            in_specs=[smem, smem, any_space, any_space, any_space],
            out_specs=pl.BlockSpec(memory_space=pltpu.VMEM),
            scratch_shapes=[
                pltpu.VMEM((ne, height, breadth), jnp.bfloat16),
                pltpu.VMEM((R, bpd * states, breadth), jnp.bfloat16),
                pltpu.VMEM((R, bpd * states, height), jnp.bfloat16),
                pltpu.VMEM((2, rows, breadth), jnp.float32),
                pltpu.VMEM((2, rows, breadth), jnp.float32),
                pltpu.VMEM((ne, states, LANES), jnp.float32),
                pltpu.VMEM((Z, flat, wide), jnp.float32),
                pltpu.VMEM((max(Z - 1, 1), flat, wide), jnp.float32),
                pltpu.VMEM((R, flat, wide), jnp.float32),
                pltpu.VMEM((max(Z - 1, 1), R // Z * bpd * states, height), jnp.bfloat16),
                pltpu.VMEM((ne, pair_rows, height), jnp.bfloat16),
                pltpu.VMEM((pair_rows, breadth), jnp.bfloat16),
                dma((2, 2)), dma, dma((2 * units,)), dma((units,)), dma((units,)),
                dma((units,)), dma((units,)),
                dma((Z,)), dma((Z,)), dma((R,)), dma((R,)),
                dma((R * bpd,)), dma((R * bpd,)), dma((R * bpd,)),
            ],
            compiler_params=pltpu.CompilerParams(
                collective_id=0, has_side_effects=True, vmem_limit_bytes=63 * 1024 * 1024 + 512 * 1024),
            name="pole_sigma",
        )(frequency_grid, band_energy, eps_static, eps_imag,
          pair_elements.reshape(bpd * states, breadth))

    return jax.shard_map(
        shards,
        mesh=mesh,
        in_specs=(P("grow", "gcol"), P("grow", "gcol"), P(), P(), P("grow", None, "gcol")),
        out_specs=P(None, "gcol"),
        check_vma=False,
    )
```
